32 devices in a mesh: ep: 8 (over z, y), tp: 4 (over x, core).
Axes of the slice: x: 2, y: 2, z: 4, core: 2. Of those that a mesh axis runs over, the one named last changes fastest.
Arguments:
- tokens: bfloat16 [256, 6144], P('ep', 'tp'), may hold values from -6 to 6
- expert_ids: int32 [256, 2], P('ep'), may hold values from 0 to 7, all different within a row; in each aligned block of 32 rows (0 to 31, 32 to 63, ...) at most 16 rows name the same one
- combine_weights: float32 [256, 2], P('ep'), may hold values from 0.1 to 1
- gate_codes: bfloat16 [6144, 65536], P(None, ('ep', 'tp')), may hold values from -6 to 6, as said below
- gate_scales: bfloat16 [192, 65536], P(None, ('ep', 'tp')), as said below
- up_codes: bfloat16 [6144, 65536], P(None, ('ep', 'tp')), may hold values from -6 to 6, as said below
- up_scales: bfloat16 [192, 65536], P(None, ('ep', 'tp')), as said below
- down_codes: bfloat16 [65536, 6144], P(('ep', 'tp')), may hold values from -6 to 6, as said below
- down_scales: bfloat16 [2048, 6144], P(('ep', 'tp')), as said below
Outputs:
- mixed: bfloat16 [256, 6144], P('ep', 'tp')
The draws below stay inside these ranges and needn't reach their ends.
Inputs may be any that keep to these rules, and one draw needn't show every extreme that they name: `expert_ids`: each token names 2 different experts. Among the 32 tokens of one index of ep no expert is named more than 16 times, a bound that some block reaches. `gate_codes`: every entry is one of 0, 0.5, 1, 1.5, 2, 3, 4, 6 or its negative. `up_codes`: every entry is one of 0, 0.5, 1, 1.5, 2, 3, 4, 6 or its negative. `down_codes`: every entry is one of 0, 0.5, 1, 1.5, 2, 3, 4, 6 or its negative. `gate_scales`: every entry is a power of two. `up_scales`: every entry is a power of two. `down_scales`: every entry is a power of two.
All inputs are finite; a program needn't handle non-finite values.
Results may differ from the reference program's by a relative error of at most 0.014.
Values may be sent and summed in bfloat16 or wider, within the bound.
No kernel may reach another device: no remote copies, remote signals or barrier semaphores. Data moves between devices by JAX's collectives and lax.ppermute only.
A program may use at most 256 MiB of HBM per device.

```python
import math
import jax
import jax.numpy as jnp
import numpy as np
from jax import lax

D = 6144
FF = 8192
EXPERTS = 8
TOPK = 2
TOK_DEV = 32
CAP = 16
FF_DEV = 2048
TOKENS = 256
N_EP = 8


code_levels = (0.0, 0.5, 1.0, 1.5, 2.0, 3.0, 4.0, 6.0, 0.0, -0.5, -1.0, -1.5, -2.0, -3.0, -4.0, -6.0)


def draw_levels(key, salt, count_rows, count_cols):
    picked = jax.random.randint(jax.random.fold_in(key, salt), (count_rows, count_cols), 0, 16)
    table = jnp.array(code_levels, jnp.float32)
    return table[picked].astype(jnp.bfloat16)


def draw_powers(key, salt, count_rows, count_cols):
    powers = jax.random.randint(jax.random.fold_in(key, salt), (count_rows, count_cols), -9, -6)
    return jnp.exp2(powers.astype(jnp.float32)).astype(jnp.bfloat16)


def draw_gate_codes(key, part):
    return draw_levels(key, 11, D, EXPERTS * FF)


def draw_up_codes(key, part):
    return draw_levels(key, 12, D, EXPERTS * FF)


def draw_down_codes(key, part):
    return draw_levels(key, 13, EXPERTS * FF, D)


def draw_gate_scales(key, part):
    return draw_powers(key, 21, D // 32, EXPERTS * FF)


def draw_up_scales(key, part):
    return draw_powers(key, 22, D // 32, EXPERTS * FF)


def draw_down_scales(key, part):
    return draw_powers(key, 23, EXPERTS * FF // 32, D)


def shard_levels(stream_key, dims, cuts, low, high):
    def one(dim, blocks):
        heights = jax.random.uniform(jax.random.fold_in(jax.random.fold_in(stream_key, 6), dim), (blocks,), jnp.float32, low / len(cuts), high / len(cuts))
        return jnp.repeat(jnp.exp(heights), dims[dim] // blocks).reshape((-1,) + (1,) * (len(dims) - dim - 1))

    loudness = one(*cuts[0])
    for cut in cuts[1:]:
        loudness = loudness * one(*cut)
    return loudness


def assign_block(rng, own, number, rows, amount, top, limit, slope):
    ranking = jax.random.permutation(rng, amount)
    crowded, ordinary = portions_of(amount, rows * top, limit, slope, True), portions_of(amount, rows * top, limit, slope, False)
    places = jnp.arange(amount)

    def named(sizes, turn):
        used = int((sizes > 0).sum())
        fixed = max(1, used // 4)
        passed = fixed + (places - fixed + turn * (used - fixed)) % max(1, amount - fixed)
        return jnp.zeros((amount,), jnp.int32).at[ranking[jnp.where(places < fixed, places, passed)]].set(jnp.asarray(sizes, jnp.int32))

    sizes = jnp.where(number % 4 == 0, named(crowded, number // 4), named(ordinary, number - number // 4 - 1))
    mixed = jax.random.permutation(jax.random.fold_in(own, 3), amount)
    giver, receiver = mixed[0:amount // 2 * 2:2], mixed[1:amount // 2 * 2:2]
    room = jnp.minimum(sizes[giver] - 1, limit - sizes[receiver]) // 2
    room = jnp.where((giver == ranking[0]) | (receiver == ranking[0]) | (sizes[receiver] == 0), 0, jnp.maximum(room, 0))
    passed = jax.random.randint(jax.random.fold_in(own, 4), (amount // 2,), 0, 1 << 20) % (room + 1)
    sizes = sizes.at[giver].add(-passed).at[receiver].add(passed)
    members = jnp.searchsorted(jnp.cumsum(sizes), jnp.arange(rows * top), side="right").astype(jnp.int32)
    grid = members.reshape(top, rows).T
    grid = grid[jax.random.permutation(jax.random.fold_in(own, 1), rows)]
    turn = jax.random.randint(jax.random.fold_in(own, 2), (rows, 1), 0, top)
    return jnp.take_along_axis(grid, (jnp.arange(top)[None, :] + turn) % top, axis=1)


def portions_of(amount, total, most, lean, full):
    loads = [(1 << 20) // math.isqrt(grade ** lean) + 1 for grade in range(1, amount + 1)]
    largest = most if full else min(most, max(-(-total // amount), total * loads[0] // sum(loads)))
    least = 1 if total - largest >= amount - 1 else 0
    holding, spare = [largest] + [least] * (amount - 1), total - largest - least * (amount - 1)
    while spare > 0:
        free = [i for i in range(1, amount) if holding[i] < largest] or [i for i in range(1, amount) if holding[i] < most]
        whole, remaining = sum([loads[i] for i in free]), spare
        for i in free:
            more = min(most - holding[i], max(1, remaining * loads[i] // whole), spare)
            holding[i] = holding[i] + more
            spare = spare - more
    return np.array(holding)


def centred(own_key, extent, deviation, bound, cuts=(), kind=jnp.bfloat16):
    values = jax.random.normal(own_key, extent, jnp.float32) * deviation
    if len(cuts) > 0:
        values = shard_levels(own_key, extent, cuts, -0.22, 0.18) * values
    return jnp.clip(values, min=-bound, max=bound).astype(kind)


def setup_inputs(seed: int = 0) -> dict:
    splits = jax.random.split(jax.random.key(seed), 10)
    tokens = centred(splits[0], (TOKENS, D), 1.0, 6.0, ((0, 8), (1, 4)))
    expert_ids_keys = jax.random.split(jax.random.fold_in(splits[1], 1), TOKENS // TOK_DEV)
    expert_ids_turns = jax.random.permutation(jax.random.fold_in(splits[1], 3), TOKENS // TOK_DEV)
    expert_ids = jax.vmap(lambda own, number: assign_block(jax.random.fold_in(splits[1], 2), own, number, TOK_DEV, EXPERTS, TOPK, CAP, 2))(expert_ids_keys, expert_ids_turns).reshape((TOKENS, TOPK))
    combine_weights = jnp.clip(0.1 + 0.9 * jax.random.uniform(splits[2], (TOKENS, TOPK), jnp.float32) ** shard_levels(splits[2], (TOKENS, TOPK), ((0, 8),), -0.2, 0.2), 0.1, 1.0)
    gate_codes = draw_gate_codes(jax.random.fold_in(splits[9], 71), 0)
    gate_scales = draw_gate_scales(jax.random.fold_in(splits[9], 71), 0)
    up_codes = draw_up_codes(jax.random.fold_in(splits[9], 71), 0)
    up_scales = draw_up_scales(jax.random.fold_in(splits[9], 71), 0)
    down_codes = draw_down_codes(jax.random.fold_in(splits[9], 71), 0)
    down_scales = draw_down_scales(jax.random.fold_in(splits[9], 71), 0)
    return {"tokens": tokens, "expert_ids": expert_ids, "combine_weights": combine_weights, "gate_codes": gate_codes, "gate_scales": gate_scales, "up_codes": up_codes, "up_scales": up_scales, "down_codes": down_codes, "down_scales": down_scales}


def dequant(code_values, scales):
    count_in, count_out = code_values.shape
    blocks = code_values.reshape(count_in // 32, 32, count_out) * scales[:, None, :]
    return blocks.reshape(count_in, count_out)


def reference(tokens, expert_ids, combine_weights, gate_codes, gate_scales, up_codes, up_scales, down_codes, down_scales):
    slot_total = N_EP * CAP
    block_ids = expert_ids.reshape(N_EP, TOK_DEV * TOPK)
    is_expert = (block_ids[:, :, None] == jnp.arange(EXPERTS, dtype=jnp.int32)[None, None, :]).astype(jnp.int32)
    before = jnp.cumsum(is_expert, axis=1) - is_expert
    slot_rank = jnp.sum(before * is_expert, axis=2)
    source = jnp.arange(N_EP, dtype=jnp.int32)[:, None]
    global_slot = (source * CAP + slot_rank).reshape(TOKENS, TOPK).astype(jnp.int32)
    slot_index = jnp.arange(slot_total, dtype=jnp.int32)

    def per_expert(mixed_sum, expert):
        keys = jnp.where(expert_ids == expert, global_slot, -1)
        chosen = jnp.zeros((slot_total, TOKENS), jnp.float32)
        weighting = jnp.zeros((TOKENS, slot_total), jnp.float32)
        for column in range(TOPK):
            match_rows = keys[:, column][None, :] == slot_index[:, None]
            chosen = chosen + match_rows.astype(jnp.float32)
            weighting = weighting + combine_weights[:, column][:, None] * jnp.transpose(match_rows).astype(jnp.float32)
        slot_rows = jnp.dot(chosen.astype(jnp.bfloat16), tokens, preferred_element_type=jnp.float32).astype(jnp.bfloat16)
        start = (expert * FF).astype(jnp.int32)
        start_block = (expert * (FF // 32)).astype(jnp.int32)
        gate_matrix = dequant(lax.dynamic_slice_in_dim(gate_codes, start, FF, 1), lax.dynamic_slice_in_dim(gate_scales, start, FF, 1))
        up_matrix = dequant(lax.dynamic_slice_in_dim(up_codes, start, FF, 1), lax.dynamic_slice_in_dim(up_scales, start, FF, 1))
        down_matrix = dequant(lax.dynamic_slice_in_dim(down_codes, start, FF, 0), lax.dynamic_slice_in_dim(down_scales, start_block, FF // 32, 0))
        gate_proj = jnp.dot(slot_rows, gate_matrix, preferred_element_type=jnp.float32)
        up_proj = jnp.dot(slot_rows, up_matrix, preferred_element_type=jnp.float32)
        hidden = (jax.nn.silu(gate_proj) * up_proj).astype(jnp.bfloat16)

        def add_block(total, block):
            lower = (block * FF_DEV).astype(jnp.int32)
            piece = lax.dynamic_slice_in_dim(hidden, lower, FF_DEV, 1)
            block_weights = lax.dynamic_slice_in_dim(down_matrix, lower, FF_DEV, 0)
            rounded = lax.optimization_barrier(jnp.dot(piece, block_weights, preferred_element_type=jnp.float32).astype(jnp.bfloat16))
            return total + rounded.astype(jnp.float32), None

        expert_out, _ = lax.scan(add_block, jnp.zeros((slot_total, D), jnp.float32), jnp.arange(FF // FF_DEV, dtype=jnp.int32))
        added = jnp.dot(weighting, expert_out, precision=lax.Precision.HIGHEST, preferred_element_type=jnp.float32)
        return mixed_sum + added, None

    mixed_sum, _ = lax.scan(per_expert, jnp.zeros((TOKENS, D), jnp.float32), jnp.arange(EXPERTS, dtype=jnp.int32))
    return mixed_sum.astype(jnp.bfloat16)
```

```python
import jax
import jax.numpy as jnp
from jax import lax
from jax.experimental import pallas as pl
from jax.experimental.pallas import tpu as pltpu
from jax.sharding import PartitionSpec as P

EXPERTS = 8
CAP = 16
BLOCK = 32
GROUPS = 2
RING = 3
KEPT = 3
FETCH_FLOPS = 4 * 10**9
MIB = 1 << 20


VMEM = pl.BlockSpec(memory_space=pltpu.VMEM)
SMEM = pl.BlockSpec(memory_space=pltpu.SMEM)
HBM = pl.BlockSpec(memory_space=pltpu.HBM)


def in_hbm(value):
    return pltpu.with_memory_space_constraint(value, pltpu.HBM)


def largest_tile(extent, most):
    return max(w for w in range(128, most + 1, 128) if extent % w == 0)


def dequant(codes, scales):
    count_in, count_out = codes.shape
    spread = jnp.broadcast_to(
        scales.astype(jnp.float32)[:, None, :], (count_in // BLOCK, BLOCK, count_out)
    ).astype(jnp.bfloat16)
    return (codes.reshape(count_in // BLOCK, BLOCK, count_out) * spread).reshape(codes.shape)


def slot_choice(ids, me, count_ep):
    count_tokens, count_top = ids.shape
    count_slots = count_ep * CAP
    lane = lax.broadcasted_iota(jnp.int32, (count_tokens, count_slots), 1)
    expert = (me ^ (lane // CAP)) // (count_ep // EXPERTS)
    named = jnp.zeros((count_tokens, count_slots), jnp.float32)
    for column in range(count_top):
        named = named + (ids[:, column : column + 1] == expert).astype(jnp.float32)
    row = lax.broadcasted_iota(jnp.int32, (count_tokens, count_tokens), 0)
    earlier = lax.broadcasted_iota(jnp.int32, (count_tokens, count_tokens), 1) < row
    rank = jnp.dot(
        earlier.astype(jnp.float32).astype(jnp.bfloat16),
        named.astype(jnp.bfloat16),
        preferred_element_type=jnp.float32,
    )
    place = (lane % CAP).astype(jnp.float32)
    return jnp.where(rank == place, named, 0.0), expert


def pack(tokens, ids, count_ep):
    width = tokens.shape[1]

    def kernel(ids_ref, tokens_ref, *out_refs):
        chosen, _ = slot_choice(ids_ref[...], lax.axis_index("ep"), count_ep)
        rows = lax.dot_general(
            chosen.astype(jnp.bfloat16),
            tokens_ref[...],
            (((0,), (0,)), ((), ())),
            preferred_element_type=jnp.float32,
        ).astype(jnp.bfloat16)
        for k, out_ref in enumerate(out_refs):
            out_ref[...] = rows[k * CAP : (k + 1) * CAP]

    return pl.pallas_call(
        kernel,
        out_shape=[jax.ShapeDtypeStruct((CAP, width), tokens.dtype)] * count_ep,
        in_specs=[VMEM, VMEM],
        out_specs=[VMEM] * count_ep,
        compiler_params=pltpu.CompilerParams(vmem_limit_bytes=8 * MIB),
        name="pack",
    )(ids, tokens)


def join(blocks):
    rows = blocks[0].shape[0]

    def kernel(*refs):
        for k, ref in enumerate(refs[:-1]):
            refs[-1][pl.ds(k * rows, rows)] = ref[...]

    return pl.pallas_call(
        kernel,
        out_shape=jax.ShapeDtypeStruct((rows * len(blocks), blocks[0].shape[1]), blocks[0].dtype),
        in_specs=[VMEM] * len(blocks),
        out_specs=VMEM,
        compiler_params=pltpu.CompilerParams(vmem_limit_bytes=2 * MIB),
        name="join",
    )(*blocks)


def add_split(here, came, rows):
    count = here.shape[0] // rows

    def kernel(here_ref, came_ref, *out_refs):
        for k, out_ref in enumerate(out_refs):
            part = pl.ds(k * rows, rows)
            out_ref[...] = (
                here_ref[part].astype(jnp.float32) + came_ref[part].astype(jnp.float32)
            ).astype(out_ref.dtype)

    return pl.pallas_call(
        kernel,
        out_shape=[jax.ShapeDtypeStruct((rows, here.shape[1]), here.dtype)] * count,
        in_specs=[VMEM, VMEM],
        out_specs=[VMEM] * count,
        compiler_params=pltpu.CompilerParams(vmem_limit_bytes=16 * MIB),
        name="add_split",
    )(here, came)


def combine(blocks, ids, weights):
    count_ep = len(blocks)
    count_tokens, count_top = ids.shape

    def kernel(ids_ref, weights_ref, *refs):
        ids_here = ids_ref[...]
        chosen, expert = slot_choice(ids_here, lax.axis_index("ep"), count_ep)
        share = jnp.zeros_like(chosen)
        for column in range(count_top):
            share = share + jnp.where(
                ids_here[:, column : column + 1] == expert, weights_ref[:, column : column + 1], 0.0
            )
        share = share * chosen
        upper = share.astype(jnp.bfloat16)
        lower = (share - upper.astype(jnp.float32)).astype(jnp.bfloat16)
        rows = jnp.concatenate([ref[...] for ref in refs[:-1]], axis=0)
        refs[-1][...] = (
            jnp.dot(upper, rows, preferred_element_type=jnp.float32)
            + jnp.dot(lower, rows, preferred_element_type=jnp.float32)
        ).astype(refs[-1].dtype)

    return pl.pallas_call(
        kernel,
        out_shape=jax.ShapeDtypeStruct((count_tokens, blocks[0].shape[1]), jnp.bfloat16),
        in_specs=[VMEM] * (2 + count_ep),
        out_specs=VMEM,
        compiler_params=pltpu.CompilerParams(vmem_limit_bytes=16 * MIB),
        name="combine",
    )(ids, weights, *blocks)


def row_copies(source, target, order_ref, sems, parts):
    rows = source.shape[0] // parts
    return [
        pltpu.make_async_copy(
            source.at[pl.ds(pl.multiple_of(order_ref[part] * rows, rows), rows)],
            target.at[pl.ds(part * rows, rows)],
            sems.at[part],
        )
        for part in range(parts)
    ]


def fetch(codes, scales, tiles, tile, order, name):
    parts = order.shape[0]
    sources = [(array, t * tile, tile) for t in tiles for array in codes]
    sources += [(array, 0, array.shape[1]) for array in scales]

    def kernel(order_ref, *refs):
        inputs, targets, sems = refs[: len(sources)], refs[len(sources) : -1], refs[-1]
        copies = []
        for n, (_, start, columns) in enumerate(sources):
            copies += row_copies(
                inputs[n].at[:, pl.ds(start, columns)], targets[n], order_ref, sems.at[n], parts
            )
        for copy in copies:
            copy.start()
        for copy in copies:
            copy.wait()

    return pl.pallas_call(
        kernel,
        out_shape=tuple(
            pltpu.VMEM((array.shape[0], columns), array.dtype) for array, _, columns in sources
        ),
        in_specs=[SMEM] + [HBM] * len(sources),
        out_specs=(VMEM,) * len(sources),
        scratch_shapes=[pltpu.SemaphoreType.DMA((len(sources), parts))],
        cost_estimate=pl.CostEstimate(
            flops=FETCH_FLOPS * len(tiles),
            bytes_accessed=len(tiles) * codes[0].shape[0] * tile * 4,
            transcendentals=0,
        ),
        compiler_params=pltpu.CompilerParams(vmem_limit_bytes=MIB // 2),
        name=name,
    )(order, *[in_hbm(array) for array, _, _ in sources])


def expert_mlp(pieces, kept, gate_s, up_s, gate_codes, up_codes, down_codes, down_scales, order):
    parts = order.shape[0]
    count_groups = len(pieces)
    group_rows, part_width = pieces[0][0].shape
    count_rows = count_groups * group_rows
    width = parts * part_width
    units = gate_codes.shape[1]
    tile = kept[0].shape[1]
    kept_tiles = len(kept) // 2
    streamed = units // tile - kept_tiles
    chunk = largest_tile(part_width, 512)
    per_part = part_width // chunk
    chunks = width // chunk
    ring = min(RING, chunks)
    half = chunks // 2
    batch = max(n for n in range(1, ring + 1) if half % n == 0)

    def kernel(order_ref, *refs):
        pieces_refs, refs = refs[: count_groups * parts], refs[count_groups * parts :]
        refs = refs[2 * kept_tiles :]
        gate_s, up_s, gate_hbm, up_hbm, down_hbm, down_s, send_ref, keep_ref = refs[:8]
        kept_refs, refs = refs[8 : 8 + 2 * kept_tiles], refs[8 + 2 * kept_tiles :]
        rows_ref, hidden, held, chunk_sems, next_sems = refs
        slots = [held.at[n] for n in range(ring)]
        started = {}

        def columns(c):
            c = (c + half) % chunks
            return pl.ds(
                pl.multiple_of(
                    order_ref[c // per_part] * part_width + (c % per_part) * chunk, chunk
                ),
                chunk,
            )

        def fill():
            while slots and len(started) < chunks:
                c, slot = len(started), slots.pop(0)
                copy = pltpu.make_async_copy(down_hbm.at[:, columns(c)], slot, chunk_sems.at[c])
                copy.start()
                started[c] = copy, slot

        def next_copies(n):
            source = pl.ds((kept_tiles + n) * tile, tile)
            return row_copies(
                gate_hbm.at[:, source], kept_refs[2 * n], order_ref, next_sems.at[n, 0], parts
            ) + row_copies(
                up_hbm.at[:, source], kept_refs[2 * n + 1], order_ref, next_sems.at[n, 1], parts
            )

        always = order_ref[0] >= 0
        fill()
        for n, ref in enumerate(pieces_refs):
            rows_ref[
                pl.ds(n // parts * group_rows, group_rows), pl.ds(n % parts * part_width, part_width)
            ] = ref[...]

        for t in range(units // tile):
            if t >= kept_tiles:
                for copy in next_copies(t - kept_tiles):
                    copy.wait()
            gate_ref, up_ref = kept_refs[2 * (t % kept_tiles)], kept_refs[2 * (t % kept_tiles) + 1]

            @pl.when(always)
            def _(cols=pl.ds(t * tile, tile), gate_ref=gate_ref, up_ref=up_ref):
                x = rows_ref[...]
                gate = jnp.dot(
                    x, dequant(gate_ref[...], gate_s[:, cols]), preferred_element_type=jnp.float32
                )
                up = jnp.dot(
                    x, dequant(up_ref[...], up_s[:, cols]), preferred_element_type=jnp.float32
                )
                hidden[:, cols] = (jax.nn.silu(gate) * up).astype(hidden.dtype)

            if t < streamed:
                for copy in next_copies(t):
                    copy.start()
            elif tile == chunk:
                for ref in (gate_ref, up_ref):
                    slots += [
                        ref.at[pl.ds(n * units, units)] for n in range(ref.shape[0] // units)
                    ]
                fill()

        for c in range(0, chunks, batch):
            for n in range(c, c + batch):
                started[n][0].wait()

            @pl.when(always)
            def _(c=c):
                for n in range(c, c + batch):
                    out_ref = send_ref if n < half else keep_ref
                    out_ref[:, pl.ds(n % half * chunk, chunk)] = jnp.dot(
                        hidden[...],
                        dequant(started[n][1][...], down_s[:, columns(n)]),
                        preferred_element_type=jnp.float32,
                    ).astype(out_ref.dtype)

            slots += [started[n][1] for n in range(c, c + batch)]
            fill()

    out = jax.ShapeDtypeStruct((count_rows, width // 2), jnp.bfloat16)
    first = 1 + count_groups * parts
    scoped = 2 * (units * ring * chunk + count_rows * (units + width)) + 3 * MIB
    return pl.pallas_call(
        kernel,
        out_shape=(out, out) + tuple(pltpu.VMEM(array.shape, array.dtype) for array in kept),
        in_specs=[SMEM] + [VMEM] * (count_groups * parts + len(kept) + 2) + [HBM] * 3 + [VMEM],
        out_specs=(VMEM,) * (2 + len(kept)),
        input_output_aliases={first + n: 2 + n for n in range(len(kept))},
        scratch_shapes=[
            pltpu.VMEM((count_rows, width), jnp.bfloat16),
            pltpu.VMEM((count_rows, units), jnp.bfloat16),
            pltpu.VMEM((ring, units, chunk), down_codes.dtype),
            pltpu.SemaphoreType.DMA((chunks,)),
            pltpu.SemaphoreType.DMA((max(streamed, 1), 2, parts)),
        ],
        cost_estimate=pl.CostEstimate(
            flops=6 * count_rows * units * width,
            bytes_accessed=down_codes.size * 2,
            transcendentals=count_rows * units,
        ),
        compiler_params=pltpu.CompilerParams(vmem_limit_bytes=scoped),
        name="expert_mlp",
    )(
        order,
        *[piece for group in pieces for piece in group],
        *kept,
        gate_s, up_s,
        in_hbm(gate_codes), in_hbm(up_codes), in_hbm(down_codes), down_scales,
    )


def per_device(
    tokens,
    expert_ids,
    combine_weights,
    gate_codes,
    gate_scales,
    up_codes,
    up_scales,
    down_codes,
    down_scales,
):
    count_ep = lax.axis_size("ep")
    count_tp = lax.axis_size("tp")
    bits = [1 << n for n in reversed(range(count_tp.bit_length() - 1))]
    places = [0]
    for bit in bits:
        places = places + [place ^ bit for place in places]
    order = jnp.array(places, jnp.int32) ^ lax.axis_index("tp").astype(jnp.int32)
    units = gate_codes.shape[1]
    tile = largest_tile(units, 512)
    kept_tiles = min(KEPT, units // tile)

    def swap(value, axis, bit):
        return lax.ppermute(value, axis, [(i, i ^ bit) for i in range(lax.axis_size(axis))])

    codes = (gate_codes, up_codes)
    *kept, gate_s, up_s = fetch(codes, (gate_scales, up_scales), [0], tile, order, "fetch_first")
    if kept_tiles > 1:
        kept += fetch(codes, (), range(1, kept_tiles), tile, order, "fetch_rest")

    blocks = pack(tokens, expert_ids, count_ep)
    came = [blocks[0]] + [swap(blocks[k], "ep", k) for k in range(1, count_ep)]
    per_group = count_ep // GROUPS
    pieces = []
    for g in range(GROUPS):
        group = [join(came[g * per_group : (g + 1) * per_group])]
        for bit in bits:
            group = group + [swap(piece, "tp", bit) for piece in group]
        pieces.append(group)

    send, keep, *_ = expert_mlp(
        pieces, kept, gate_s, up_s, gate_codes, up_codes, down_codes, down_scales, order
    )
    rows = per_group * CAP
    for bit in reversed(bits[1:]):
        got = swap(send, "tp", bit)
        terms = (keep.astype(jnp.float32) + got.astype(jnp.float32)).astype(jnp.bfloat16)
        half = terms.shape[1] // 2
        keep, send = terms[:, :half], terms[:, half:]
    back = []
    for g in range(GROUPS):
        part = slice(g * rows, (g + 1) * rows)
        back = back + list(add_split(keep[part], swap(send[part], "tp", bits[0]), CAP))
    back = [back[0]] + [swap(back[k], "ep", k) for k in range(1, count_ep)]
    return combine(back, expert_ids, combine_weights)


def solution(mesh):
    placed = (
        P("ep", "tp"),
        P("ep", None),
        P("ep", None),
        P(None, ("ep", "tp")),
        P(None, ("ep", "tp")),
        P(None, ("ep", "tp")),
        P(None, ("ep", "tp")),
        P(("ep", "tp"), None),
        P(("ep", "tp"), None),
    )
    return jax.shard_map(
        per_device, mesh=mesh, in_specs=placed, out_specs=P("ep", "tp"), check_vma=False
    )
```
